32 devices in a mesh: bank: 4 (over y, x), zero: 8 (over z, core).
Axes of the slice: x: 2, y: 2, z: 4, core: 2. Of those that a mesh axis runs over, the one named last changes fastest.
Arguments:
- w_down: float32 [64, 1024, 2048], P('bank', None, 'zero'), may hold values from -0.25 to 0.25
- avg_down: bfloat16 [64, 1024, 2048], P('bank', None, 'zero'), may hold values from -0.09375 to 0.09375
- router_weight: float32 [2048, 64], P('zero', 'bank'), may hold values from -0.125 to 0.125
- router_gain: float32 [2048], P('zero'), may hold values from 0.25 to 1.75
Outputs:
- serve_down: bfloat16 [64, 1024, 2048], P('bank')
- scale_down: float32 [64, 1024], P('bank')
- serve_router: bfloat16 [2048, 64], replicated
The draws below stay inside these ranges and needn't reach their ends.
All inputs are finite; a program needn't handle non-finite values.
Results may differ from the reference program's by a relative error of at most 0.001.
Values may be sent and summed in bfloat16 or wider, within the bound.
A program may use at most 256 MiB of HBM per device.

```python
import jax
import jax.numpy as jnp
from jax import lax

EXPERTS = 64
D_MODEL = 2048
D_EXPERT = 1024


def strengthened(values, key, source, target, parts, factor):
    def block_of(position):
        return (jnp.arange(values.shape[position]) // (values.shape[position] // parts)).reshape((-1,) + (1,) * (values.ndim - 1 - position))

    one_side = jax.random.permutation(key, parts)[block_of(target)]
    far = (block_of(target) + parts // 2) % parts
    return jnp.where((block_of(source) == one_side) | (block_of(source) == far), factor * values, values)


def block_levels(key, extent, shards, least, largest):
    gain, own = 1.0, jax.random.fold_in(key, 6)
    for dim, parts in shards:
        steps = jnp.exp(jax.random.uniform(jax.random.fold_in(own, dim), (parts,), jnp.float32, least / len(shards), largest / len(shards)))
        gain = gain * jnp.repeat(steps, extent[dim] // parts).reshape([-1 if axis == dim else 1 for axis in range(len(extent))])
    return gain


def scatter_about(own_key, dims, spread, limit, cuts=(), dtype=jnp.bfloat16):
    array = jax.random.normal(own_key, dims, jnp.float32) * spread
    if len(cuts) > 0:
        array = block_levels(own_key, dims, cuts, -0.22, 0.18) * array
    return jnp.clip(array, min=-limit, max=limit).astype(dtype)


def gaussian_with(rng, dims, width, bound, cuts, heavy, kind=jnp.bfloat16):
    array = width * jax.random.normal(rng, dims, jnp.float32)
    if cuts:
        array = array * block_levels(rng, dims, cuts, -0.22, 0.18)
    return jnp.clip(strengthened(array, jax.random.fold_in(rng, 3), *heavy), -bound, bound).astype(kind)


def setup_inputs(seed: int = 0) -> dict:
    key_of = jax.random.split(jax.random.key(seed), 5)
    return {
        "w_down": gaussian_with(key_of[0], (EXPERTS, D_EXPERT, D_MODEL), D_EXPERT ** -0.5, 0.25, ((0, 4), (2, 8)), (2, 1, 8, 2.0), jnp.float32),
        "avg_down": scatter_about(key_of[1], (EXPERTS, D_EXPERT, D_MODEL), (D_EXPERT * 4) ** -0.5, 0.09375, ((0, 4), (2, 8))),
        "router_weight": scatter_about(key_of[2], (D_MODEL, EXPERTS), D_MODEL ** -0.5, 0.125, ((0, 8), (1, 4)), jnp.float32),
        "router_gain": jnp.clip(1.0 + 0.15 * jax.random.normal(key_of[3], (D_MODEL,), jnp.float32), 0.25, 1.75),
    }


def reference(w_down, avg_down, router_weight, router_gain):
    fresh_down = w_down + avg_down.astype(jnp.float32)
    scale_down = jnp.sqrt(lax.optimization_barrier(jnp.sum(fresh_down * fresh_down, axis=2)))
    serve_down = (fresh_down / jnp.expand_dims(scale_down, 2)).astype(jnp.bfloat16)
    serve_router = (router_weight * router_gain[:, None]).astype(jnp.bfloat16)
    return (serve_down, scale_down, serve_router)
```

```python
import functools

import jax
import jax.numpy as jnp
from jax import lax
from jax.experimental import pallas as pl
from jax.experimental.pallas import tpu as pltpu
from jax.sharding import PartitionSpec as P

MESH = pl.DeviceIdType.MESH


def exchange_kernel(n, part_ref, out_ref, held, send_sems, recv_sems):
    bank, me = lax.axis_index("bank"), lax.axis_index("zero")
    barrier = pltpu.get_barrier_semaphore()
    for k in range(1, n):
        pl.semaphore_signal(barrier, inc=1, device_id=(bank, lax.rem(me + k, n)), device_id_type=MESH)
    pl.semaphore_wait(barrier, n - 1)
    copies = []
    for k in range(1, n):
        copy = pltpu.make_async_remote_copy(
            src_ref=part_ref,
            dst_ref=held.at[k - 1],
            send_sem=send_sems.at[k - 1],
            recv_sem=recv_sems.at[k - 1],
            device_id=(bank, lax.rem(me + k, n)),
            device_id_type=MESH,
        )
        copy.start()
        copies.append(copy)
    for copy in copies:
        copy.wait()
    total = jnp.zeros(part_ref.shape, jnp.float32)
    for d in range(n):
        slot = lax.rem(me - d + n, n)
        other = held[jnp.maximum(slot - 1, 0)]
        total += jnp.where(slot == 0, part_ref[...], other)
    out_ref[...] = total


def exchange(part, n, cid):
    rows = part.shape
    return pl.pallas_call(
        functools.partial(exchange_kernel, n),
        out_shape=jax.ShapeDtypeStruct(rows, jnp.float32),
        in_specs=[pl.BlockSpec(memory_space=pltpu.VMEM)],
        out_specs=pl.BlockSpec(memory_space=pltpu.VMEM),
        scratch_shapes=[
            pltpu.VMEM((n - 1,) + rows, jnp.float32),
            pltpu.SemaphoreType.DMA((n - 1,)),
            pltpu.SemaphoreType.DMA((n - 1,)),
        ],
        compiler_params=pltpu.CompilerParams(collective_id=cid, has_side_effects=True),
        cost_estimate=pl.CostEstimate(flops=1000, bytes_accessed=20_000_000, transcendentals=0),
        name=f"exchange_{cid}",
    )(part)


def place_kernel(src_ref, *refs):
    refs[-1][...] = src_ref[0]


def place(gathered, base, start, shape):
    n, rows, cols = gathered.shape
    block = 256
    while rows % block or start % block:
        block //= 2
    for bigger in (2048, 1024, 512):
        if rows % bigger == 0 and start % bigger == 0:
            block = bigger
            break
    operands, specs, aliases = [gathered], [pl.BlockSpec((1, block, cols), lambda r, d: (d, r, 0))], {}
    if base is not None:
        operands.append(base)
        specs.append(pl.BlockSpec(memory_space=pl.ANY))
        aliases = {1: 0}
    first = start // block
    return pl.pallas_call(
        place_kernel,
        grid=(rows // block, n),
        out_shape=jax.ShapeDtypeStruct(shape, gathered.dtype),
        in_specs=specs,
        out_specs=pl.BlockSpec((block, cols), lambda r, d: (first + r, d)),
        input_output_aliases=aliases,
        cost_estimate=pl.CostEstimate(flops=0, bytes_accessed=4 * gathered.size, transcendentals=0),
        name=f"place_{start}",
    )(*operands)


def shards(n, w_down, avg_down, router_weight, router_gain):
    experts, inner, cols = w_down.shape
    rows = experts * inner
    w = w_down.reshape(rows, cols)
    a = avg_down.reshape(rows, cols)
    edge = rows // 16
    cuts = [0, edge, rows - edge, rows]

    def sums(w, a, cid):
        fresh = w + a.astype(jnp.float32)
        part = jnp.sum(fresh * fresh, axis=1).reshape(-1, 128)
        return jnp.sqrt(exchange(part, n, cid)).reshape(-1)

    def narrow(w, a, scale):
        return ((w + a.astype(jnp.float32)) / scale[:, None]).astype(jnp.bfloat16)

    def gather(x):
        return lax.all_gather(x, "zero", axis=0)

    scale_0 = sums(w[:edge], a[:edge], 0)
    narrow_0 = narrow(w[:edge], a[:edge], scale_0)
    narrow_0, w, a, router_weight = lax.optimization_barrier((narrow_0, w, a, router_weight))
    gathered_0 = gather(narrow_0)
    scale_1 = sums(w[edge:], a[edge:], 1)
    mid = rows - 2 * edge
    narrow_1 = narrow(w[edge:-edge], a[edge:-edge], scale_1[:mid])
    narrow_2 = narrow(w[-edge:], a[-edge:], scale_1[mid:])
    gathered_1 = gather(narrow_1)
    gathered_2 = gather(narrow_2)
    shape = (rows, cols * n)
    out = place(gathered_0, None, 0, shape)
    out = place(gathered_1, out, edge, shape)
    out = place(gathered_2, out, rows - edge, shape)
    serve_down = out.reshape(experts, inner, cols * n)
    scale_down = jnp.concatenate([scale_0, scale_1]).reshape(experts, inner)
    part_router = (router_weight * router_gain[:, None]).astype(jnp.bfloat16)
    row_router = lax.all_gather(part_router, "zero", axis=0, tiled=True)
    serve_router = lax.all_gather(row_router, "bank", axis=1, tiled=True)
    return (serve_down, scale_down, serve_router)


def solution(mesh):
    return jax.shard_map(
        functools.partial(shards, mesh.shape["zero"]),
        mesh=mesh,
        in_specs=(P("bank", None, "zero"), P("bank", None, "zero"), P("zero", "bank"), P("zero")),
        out_specs=(P("bank", None, None), P("bank", None), P()),
        check_vma=False,
    )
```

```python
import functools

import jax
import jax.numpy as jnp
from jax import lax
from jax.experimental import pallas as pl
from jax.experimental.pallas import tpu as pltpu
from jax.sharding import PartitionSpec as P

MESH = pl.DeviceIdType.MESH


def exchange_kernel(n, part_ref, out_ref, held, send_sems, recv_sems):
    bank, me = lax.axis_index("bank"), lax.axis_index("zero")
    barrier = pltpu.get_barrier_semaphore()
    for k in range(1, n):
        pl.semaphore_signal(barrier, inc=1, device_id=(bank, lax.rem(me + k, n)), device_id_type=MESH)
    pl.semaphore_wait(barrier, n - 1)
    copies = []
    for k in range(1, n):
        copy = pltpu.make_async_remote_copy(
            src_ref=part_ref,
            dst_ref=held.at[k - 1],
            send_sem=send_sems.at[k - 1],
            recv_sem=recv_sems.at[k - 1],
            device_id=(bank, lax.rem(me + k, n)),
            device_id_type=MESH,
        )
        copy.start()
        copies.append(copy)
    for copy in copies:
        copy.wait()
    total = jnp.zeros(part_ref.shape, jnp.float32)
    for d in range(n):
        slot = lax.rem(me - d + n, n)
        other = held[jnp.maximum(slot - 1, 0)]
        total += jnp.where(slot == 0, part_ref[...], other)
    out_ref[...] = total


def exchange(part, n, cid):
    rows = part.shape
    return pl.pallas_call(
        functools.partial(exchange_kernel, n),
        out_shape=jax.ShapeDtypeStruct(rows, jnp.float32),
        in_specs=[pl.BlockSpec(memory_space=pltpu.VMEM)],
        out_specs=pl.BlockSpec(memory_space=pltpu.VMEM),
        scratch_shapes=[
            pltpu.VMEM((n - 1,) + rows, jnp.float32),
            pltpu.SemaphoreType.DMA((n - 1,)),
            pltpu.SemaphoreType.DMA((n - 1,)),
        ],
        compiler_params=pltpu.CompilerParams(collective_id=cid, has_side_effects=True),
        cost_estimate=pl.CostEstimate(flops=1000, bytes_accessed=20_000_000, transcendentals=0),
        name=f"exchange_{cid}",
    )(part)


def exchange_two_kernel(n, part_ref, out_ref, held, own, gathered, send_sems, recv_sems, send_sems_2, recv_sems_2):
    bank, me = lax.axis_index("bank"), lax.axis_index("zero")
    barrier = pltpu.get_barrier_semaphore()
    for k in range(1, n):
        pl.semaphore_signal(barrier, inc=1, device_id=(bank, lax.rem(me + k, n)), device_id_type=MESH)
    pl.semaphore_wait(barrier, n - 1)
    scatter = []
    for k in range(1, n):
        peer = lax.rem(me + k, n)
        copy = pltpu.make_async_remote_copy(
            src_ref=part_ref.at[peer],
            dst_ref=held.at[k - 1],
            send_sem=send_sems.at[k - 1],
            recv_sem=recv_sems.at[k - 1],
            device_id=(bank, peer),
            device_id_type=MESH,
        )
        copy.start()
        scatter.append(copy)
    total = part_ref[me]
    for k in range(1, n):
        scatter[k - 1].wait_recv()
        total += held[k - 1]
    own[...] = total
    out_ref[me] = total
    for copy in scatter:
        copy.wait_send()
    spread = []
    for k in range(1, n):
        copy = pltpu.make_async_remote_copy(
            src_ref=own,
            dst_ref=gathered.at[k - 1],
            send_sem=send_sems_2.at[k - 1],
            recv_sem=recv_sems_2.at[k - 1],
            device_id=(bank, lax.rem(me + k, n)),
            device_id_type=MESH,
        )
        copy.start()
        spread.append(copy)
    for k in range(1, n):
        spread[k - 1].wait_recv()
        out_ref[lax.rem(me - k + n, n)] = gathered[k - 1]
    for copy in spread:
        copy.wait_send()


def exchange_two(part, n, cid):
    block = (part.shape[0] // n,) + part.shape[1:]
    return pl.pallas_call(
        functools.partial(exchange_two_kernel, n),
        out_shape=jax.ShapeDtypeStruct((n,) + block, jnp.float32),
        in_specs=[pl.BlockSpec(memory_space=pltpu.VMEM)],
        out_specs=pl.BlockSpec(memory_space=pltpu.VMEM),
        scratch_shapes=[
            pltpu.VMEM((n - 1,) + block, jnp.float32),
            pltpu.VMEM(block, jnp.float32),
            pltpu.VMEM((n - 1,) + block, jnp.float32),
        ]
        + [pltpu.SemaphoreType.DMA((n - 1,))] * 4,
        compiler_params=pltpu.CompilerParams(collective_id=cid, has_side_effects=True),
        cost_estimate=pl.CostEstimate(flops=1000, bytes_accessed=20_000_000, transcendentals=0),
        name=f"exchange_{cid}",
    )(part.reshape((n,) + block)).reshape(part.shape)


def place_kernel(n, src_ref, *refs):
    cols = src_ref.shape[2]
    for d in range(n):
        refs[-1][:, d * cols : (d + 1) * cols] = src_ref[d]


def place(gathered, base, start, shape):
    n, rows, cols = gathered.shape
    block = 512 if rows > 1024 else 256
    while rows % block or start % block:
        block //= 2
    operands, specs, aliases = [gathered], [pl.BlockSpec((n, block, cols), lambda r: (0, r, 0))], {}
    if base is not None:
        operands.append(base)
        specs.append(pl.BlockSpec(memory_space=pl.ANY))
        aliases = {1: 0}
    first = start // block
    return pl.pallas_call(
        functools.partial(place_kernel, n),
        grid=(rows // block,),
        out_shape=jax.ShapeDtypeStruct(shape, gathered.dtype),
        in_specs=specs,
        out_specs=pl.BlockSpec((block, n * cols), lambda r: (first + r, 0)),
        input_output_aliases=aliases,
        cost_estimate=pl.CostEstimate(flops=0, bytes_accessed=4 * gathered.size, transcendentals=0),
        name=f"place_{start}",
    )(*operands)


def shards(n, w_down, avg_down, router_weight, router_gain):
    experts, inner, cols = w_down.shape
    rows = experts * inner
    w = w_down.reshape(rows, cols)
    a = avg_down.reshape(rows, cols)
    edge = rows // 16

    def sums(w, a, cid, how):
        fresh = w + a.astype(jnp.float32)
        part = jnp.sum(fresh * fresh, axis=1).reshape(-1, 128)
        return jnp.sqrt(how(part, n, cid)).reshape(-1)

    def narrow(w, a, scale):
        return ((w + a.astype(jnp.float32)) / scale[:, None]).astype(jnp.bfloat16)

    def gather(x):
        return lax.all_gather(x, "zero", axis=0)

    scale_0 = sums(w[:edge], a[:edge], 0, exchange)
    narrow_0 = narrow(w[:edge], a[:edge], scale_0)
    narrow_0, w, a, router_weight = lax.optimization_barrier((narrow_0, w, a, router_weight))
    gathered_0 = gather(narrow_0)
    scale = sums(w, a, 1, exchange_two)
    narrow_1 = narrow(w[edge:-edge], a[edge:-edge], scale[edge:-edge])
    narrow_2 = narrow(w[-edge:], a[-edge:], scale[-edge:])
    gathered_1 = gather(narrow_1)
    gathered_2 = gather(narrow_2)
    shape = (rows, cols * n)
    out = place(gathered_0, None, 0, shape)
    out = place(gathered_1, out, edge, shape)
    out = place(gathered_2, out, rows - edge, shape)
    serve_down = out.reshape(experts, inner, cols * n)
    scale_down = scale.reshape(experts, inner)
    part_router = (router_weight * router_gain[:, None]).astype(jnp.bfloat16)
    row_router = lax.all_gather(part_router, "zero", axis=0, tiled=True)
    serve_router = lax.all_gather(row_router, "bank", axis=1, tiled=True)
    return (serve_down, scale_down, serve_router)


def solution(mesh):
    return jax.shard_map(
        functools.partial(shards, mesh.shape["zero"]),
        mesh=mesh,
        in_specs=(P("bank", None, "zero"), P("bank", None, "zero"), P("zero", "bank"), P("zero")),
        out_specs=(P("bank", None, None), P("bank", None), P()),
        check_vma=False,
    )
```
